128 devices in a mesh: batch: 1, rows: 128 (over z, y, x, core).
Axes of the slice: x: 4, y: 4, z: 4, core: 2. Of those that a mesh axis runs over, the one named last changes fastest.
Arguments:
- a_mat: float32 [262144, 1024], P(('batch', 'rows'))
- rhs: float32 [262144, 64], P(('batch', 'rows'))
Outputs:
- output 1: float32 [1024, 64], P('batch')
- output 2: float32 [1024, 1024], P('batch')
All inputs are finite; a program needn't handle non-finite values.
Results may differ from the reference program's by a relative error of at most 0.001.
Values sent between devices are 32-bit elements.
A program may use at most 1 GiB of HBM per device.

```python
import jax
import jax.numpy as jnp
from jax import lax
import math

M_ROWS = 262144
N_COLS = 1024
N_RHS = 64
SHARDS = 128
COND_NUMBER = 1000.0
NOISE_LEVEL = 0.001


def setup_inputs(seed: int = 0, part: int = 0) -> dict:
    part_key = jax.random.fold_in(jax.random.key(seed), part)
    key_base, key_mix, key_sol, key_noise = jax.random.split(part_key, 4)
    rows_per = M_ROWS // SHARDS
    base = jax.random.normal(key_base, (M_ROWS, N_COLS), jnp.float32)
    row_shard = jnp.arange(M_ROWS) // rows_per
    col_owner = jnp.arange(N_COLS) % SHARDS
    low_weight = 0.5 / math.sqrt(SHARDS)
    weights = jnp.where(row_shard[:, None] == col_owner[None, :], 1.0, low_weight)
    col_scale = 1.0 / math.sqrt(rows_per * (1.0 + 0.25 * (SHARDS - 1) / SHARDS))
    basis = base * weights * col_scale
    ortho = jnp.linalg.qr(jax.random.normal(key_mix, (N_COLS, N_COLS), jnp.float32))[0]
    tail_len = N_COLS // 4
    tail_pos = jnp.clip((jnp.arange(N_COLS) - (N_COLS - tail_len)) / (tail_len - 1), 0.0, 1.0)
    sigma = jnp.power(COND_NUMBER, -tail_pos)
    upper_c = jnp.linalg.qr(sigma[:, None] * ortho.T)[1] * math.sqrt(N_COLS)
    a_mat = jnp.dot(basis, upper_c, precision=lax.Precision.HIGHEST)
    x_true = jax.random.normal(key_sol, (N_COLS, N_RHS), jnp.float32)
    signal = jnp.dot(a_mat, x_true, precision=lax.Precision.HIGHEST)
    noise_scale = NOISE_LEVEL * jnp.sqrt(jnp.mean(signal * signal))
    rhs = signal + noise_scale * jax.random.normal(key_noise, (M_ROWS, N_RHS), jnp.float32)
    return {"a_mat": a_mat.astype(jnp.float32), "rhs": rhs.astype(jnp.float32)}


def reference(a_mat, rhs):
    highest = lax.Precision.HIGHEST
    gram_one = jnp.dot(a_mat.T, a_mat, precision=highest, preferred_element_type=jnp.float32)
    low_one = jnp.linalg.cholesky(gram_one)
    q_one = lax.linalg.triangular_solve(low_one, a_mat, left_side=False, lower=True, transpose_a=True)
    gram_two = jnp.dot(q_one.T, q_one, precision=highest, preferred_element_type=jnp.float32)
    low_two = jnp.linalg.cholesky(gram_two)
    proj_one = jnp.dot(q_one.T, rhs, precision=highest, preferred_element_type=jnp.float32)
    proj_two = lax.linalg.triangular_solve(low_two, proj_one, left_side=True, lower=True)
    upper_r = jnp.dot(low_two.T, low_one.T, precision=highest, preferred_element_type=jnp.float32)
    x_sol = lax.linalg.triangular_solve(upper_r, proj_two, left_side=True, lower=False)
    return (x_sol, upper_r)
```

```python
import functools
import jax
import jax.numpy as jnp
from jax import lax
from jax.experimental import pallas as pl
from jax.experimental.pallas import tpu as pltpu
from jax.sharding import PartitionSpec as P

HIGHEST = lax.Precision.HIGHEST
NB = 128
N = 1024
N_BLK = 8


def block_row(i, j):
    return NB * (i * 8 - i * (i - 1) // 2 + (j - i))


def dot_tn(x, y):
    return lax.dot_general(x, y, (((0,), (0,)), ((), ())), precision=HIGHEST, preferred_element_type=jnp.float32)


def pack_row(out_ref, prod, bi, col):
    for a in range(2):
        for j in range(max(2 * bi + a, col // NB), min(8, (col + prod.shape[1]) // NB)):
            at, c = block_row(2 * bi + a, j), j * NB - col
            out_ref[at:at + NB, :] = prod[a * NB:(a + 1) * NB, c:c + NB]


def gram_kernel(a_ref, out_ref):
    for bj in range(4):
        for bi in range(bj + 1):
            pack_row(out_ref, dot_tn(a_ref[:, bi * 256:(bi + 1) * 256], a_ref[:, bj * 256:(bj + 1) * 256]), bi, bj * 256)


def gram_first(a):
    vm = pl.BlockSpec(memory_space=pltpu.VMEM)
    return pl.pallas_call(gram_kernel, out_shape=jax.ShapeDtypeStruct((36 * NB, NB), jnp.float32), in_specs=[vm], out_specs=vm,
        cost_estimate=pl.CostEstimate(flops=2 * 10 * 256 * 256 * 2048, bytes_accessed=10 << 20, transcendentals=0))(a)


def factor_block(sym, fillers=()):
    n_s = len(sym)
    row_id = lax.broadcasted_iota(jnp.int32, (8, NB), 0)
    lane_id = lax.broadcasted_iota(jnp.int32, (8, NB), 1)
    left = list(sym)
    right = [jnp.where(lane_id == row_id + 8 * s, 1.0, 0.0).astype(jnp.float32) for s in range(n_s)]
    fillers = list(fillers)
    for kb in range(n_s):
        for step in fillers[kb:kb + 1] if kb < n_s - 1 else fillers[kb:]:
            step()
        col = {s: [jnp.broadcast_to(left[s][:, 8 * kb + j:8 * kb + j + 1], (8, NB)) for j in range(8)] for s in range(kb, n_s)}
        for j in range(8):
            d = jnp.broadcast_to(col[kb][j][j:j + 1, :], (8, NB))
            rs = lax.rsqrt(d)
            lcol = {s: col[s][j] * rs for s in range(kb, n_s)}
            for m in range(j + 1, 8):
                lm = jnp.broadcast_to(lcol[kb][m:m + 1, :], (8, NB))
                for s in range(kb, n_s):
                    col[s][m] = col[s][m] - lcol[s] * lm
            row_l = jnp.broadcast_to(left[kb][j:j + 1, :], (8, NB)) * rs
            row_r = jnp.broadcast_to(right[kb][j:j + 1, :], (8, NB)) * rs
            lmask = jnp.where(row_id > j, lcol[kb], 0.0)
            left[kb] = jnp.where(row_id == j, row_l, left[kb] - lmask * row_l)
            right[kb] = jnp.where(row_id == j, row_r, right[kb] - lmask * row_r)
            for s in range(kb + 1, n_s):
                left[s] = left[s] - lcol[s] * row_l
                right[s] = right[s] - lcol[s] * row_r
    left = [jnp.where(lane_id >= row_id + 8 * s, left[s], 0.0) for s in range(n_s)]
    return left, right


def dot_nn(x, y):
    return jnp.dot(x, y, precision=HIGHEST, preferred_element_type=jnp.float32)


def chol_loop(g_ref, aug_ref, r_ref, t_ref, l_ref, m_ref):
    width = r_ref.shape[1]
    for i in range(N_BLK):
        for j in range(i, N_BLK):
            t_ref[i * NB:(i + 1) * NB, j * NB:(j + 1) * NB] = g_ref[block_row(i, j):block_row(i, j) + NB, :]
    if aug_ref is not None:
        t_ref[:, N:] = aug_ref[...]

    def panel(k, carry):
        base = pl.multiple_of(k * NB, NB)
        rows = pl.ds(base, NB)
        left, right = factor_block([t_ref[pl.ds(pl.multiple_of(base + 8 * s, 8), 8), rows] for s in range(NB // 8)])
        m_ref[rows, :] = jnp.concatenate(right, axis=0)
        r_ref[rows, rows] = jnp.concatenate(left, axis=0)
        for kk in range(N_BLK):
            @pl.when(k == kk)
            def _():
                top, lo = kk * NB, (kk + 1) * NB
                if top:
                    r_ref[top:lo, :top] = jnp.zeros((NB, top), jnp.float32)
                if lo < width:
                    r_ref[top:lo, lo:] = dot_nn(m_ref[top:lo, :], t_ref[top:lo, lo:])
                for j in range(kk + 1, N_BLK):
                    l_ref[j * NB:(j + 1) * NB, :] = r_ref[top:lo, j * NB:(j + 1) * NB].T
                if lo < N:
                    for c in range(lo, width, 256):
                        end = min(c + 256, width)
                        hi = min(end, N)
                        t_ref[lo:hi, c:end] = t_ref[lo:hi, c:end] - dot_nn(l_ref[lo:hi, :], r_ref[top:lo, c:end])
        return carry

    lax.fori_loop(0, N_BLK, panel, 0)


def wide_inverse(r_ref, m_ref, x_ref):
    for j in range(N_BLK // 2):
        a, b = slice(2 * j * NB, (2 * j + 1) * NB), slice((2 * j + 1) * NB, (2 * j + 2) * NB)
        xa, xb = m_ref[a, :].T, m_ref[b, :].T
        x_ref[a, :NB] = xa
        x_ref[b, NB:] = xb
        x_ref[b, :NB] = jnp.zeros((NB, NB), jnp.float32)
        x_ref[a, NB:] = -dot_nn(dot_nn(xa, r_ref[a, b]), xb)


def middle_kernel(g_ref, a_hbm, b_ref, out_ref, r_ref, x_ref, q_ref, w_ref, l_ref, m_ref, sem):
    load = pltpu.make_async_copy(a_hbm, q_ref, sem)
    load.start()
    chol_loop(g_ref, None, r_ref, w_ref, l_ref, m_ref)
    wide_inverse(r_ref, m_ref, x_ref)
    for bj in range(4):
        lo, hi = bj * 256, (bj + 1) * 256
        if bj:
            w_ref[:lo, lo:hi] = -dot_nn(r_ref[:lo, lo:hi], x_ref[lo:hi, :])
        w_ref[lo:hi, lo:hi] = x_ref[lo:hi, :]
    load.wait()
    half = q_ref.shape[0] // 2
    for bj in range(4):
        lo, hi = bj * 256, (bj + 1) * 256
        for h in range(0, 2 * half, half):
            q_ref[h:h + half, lo:hi] = dot_nn(q_ref[h:h + half, :hi], w_ref[:hi, lo:hi])
        for bi in range(bj + 1):
            pack_row(out_ref, dot_tn(q_ref[:, bi * 256:(bi + 1) * 256], q_ref[:, lo:hi]), bi, lo)
        proj = dot_tn(q_ref[:, lo:hi], b_ref[...])
        at = 36 * NB + bj * NB
        out_ref[at:at + NB, :] = proj[:NB] + pltpu.roll(proj[NB:], 64, 1)


def middle(packed, a, b):
    vm, hbm = pl.BlockSpec(memory_space=pltpu.VMEM), pl.BlockSpec(memory_space=pl.ANY)
    v = lambda *s: pltpu.VMEM(s, jnp.float32)
    o = lambda *s: jax.ShapeDtypeStruct(s, jnp.float32)
    return pl.pallas_call(
        middle_kernel, out_shape=(o(40 * NB, NB), o(N, N), o(N, 256)),
        in_specs=[vm, hbm, vm], out_specs=(vm,) * 3,
        scratch_shapes=[v(*a.shape), v(N, N), v(N, NB), v(N, NB), pltpu.SemaphoreType.DMA],
        cost_estimate=pl.CostEstimate(flops=2 * 22 * 256 * 256 * 2048, bytes_accessed=20 << 20, transcendentals=0))(packed, a, b)


def last_kernel(g_ref, r1_ref, x1_ref, sol_ref, out_ref, r_ref, t_ref, l_ref, m_ref, aug_ref, x_ref):
    for j in range(4):
        tile = g_ref[36 * NB + j * NB:36 * NB + (j + 1) * NB, :]
        aug_ref[2 * j * NB:(2 * j + 1) * NB, :] = tile
        aug_ref[(2 * j + 1) * NB:(2 * j + 2) * NB, :] = pltpu.roll(tile, 64, 1)
    chol_loop(g_ref, aug_ref, r_ref, t_ref, l_ref, m_ref)
    wide_inverse(r_ref, m_ref, x_ref)
    for bi in reversed(range(4)):
        lo, hi = bi * 256, (bi + 1) * 256
        for bj in range(4):
            cl, ch = bj * 256, (bj + 1) * 256
            if bj < bi:
                out_ref[lo:hi, cl:ch] = jnp.zeros((256, 256), jnp.float32)
            else:
                out_ref[lo:hi, cl:ch] = dot_nn(r_ref[lo:hi, lo:ch], r1_ref[lo:ch, cl:ch])
        c = r_ref[lo:hi, N:]
        if bi < 3:
            c = c - dot_nn(out_ref[lo:hi, hi:], aug_ref[hi:, :])
        aug_ref[lo:hi, :] = dot_nn(x1_ref[lo:hi, :], dot_nn(x_ref[lo:hi, :], c))
    sol_ref[...] = aug_ref[:, :64]


def last(packed, r1, x1):
    vm = pl.BlockSpec(memory_space=pltpu.VMEM)
    v = lambda *s: pltpu.VMEM(s, jnp.float32)
    o = lambda *s: jax.ShapeDtypeStruct(s, jnp.float32)
    return pl.pallas_call(
        last_kernel, out_shape=(o(N, 64), o(N, N)), in_specs=[vm] * 3, out_specs=(vm,) * 2,
        scratch_shapes=[v(N, N + NB), v(N, N + NB), v(N, NB), v(N, NB), v(N, NB), v(N, 256)],
        cost_estimate=pl.CostEstimate(flops=2 * N ** 3, bytes_accessed=16 << 20, transcendentals=0))(packed, r1, x1)


MESH = pl.DeviceIdType.MESH
AXES = ((0, 1, 2), (1, 2, 0), (2, 0, 1))


def part_offsets(units, per_unit):
    offs, total = [], 0
    for u in units:
        offs.append(total)
        total += per_unit * u * 8
    return offs, total


def ar_kernel(units, in_ref, out_ref, h_ref, rb0, rb1, p1, rb2, p2, rb3, ssem, rsem):
    me = lax.axis_index("rows")
    core = lax.rem(me, 2)
    coord = [lax.rem(me // 2, 4), lax.rem(me // 8, 4), me // 32]
    scale = [2, 8, 32]

    def peer(axis, d):
        c = coord[axis]
        return (0, me + (lax.rem(c + d, 4) - c) * scale[axis])

    partner = (0, me + 1 - 2 * core)
    barrier = pltpu.get_barrier_semaphore()
    targets = [partner] + [peer(ax, d) for ax in range(3) for d in (1, 2, 3)]
    for t in targets:
        pl.semaphore_signal(barrier, inc=1, device_id=t, device_id_type=MESH)
    pl.semaphore_wait(barrier, len(targets))

    hoff, hn = part_offsets(units, 16)
    off1, _ = part_offsets(units, 12)
    offp1, _ = part_offsets(units, 4)
    off2, _ = part_offsets(units, 3)
    offp2, _ = part_offsets(units, 1)
    mine, other = core * hn, (1 - core) * hn
    order = (2, 1, 3, 0)
    sends = []

    def rows(start, size):
        return pl.ds(pl.multiple_of(start, 8), size)

    def copy(src, dst, sem, target):
        return pltpu.make_async_remote_copy(src_ref=src, dst_ref=dst, send_sem=ssem.at[sem], recv_sem=rsem.at[sem], device_id=target, device_id_type=MESH)

    def send(src, dst, sem, target):
        c = copy(src, dst, sem, target)
        c.start()
        sends.append(c)

    n_p = len(units)

    def sem_of(phase, p, d):
        return (phase * n_p + p) * 4 + d

    def achunk(p, d):
        return lax.rem(coord[AXES[p][0]] + d, 4)

    def bchunk(p, d):
        return lax.rem(coord[AXES[p][1]] + d, 4)

    for d in order:
        for p in range(n_p):
            cs = 32 * units[p]
            at = hoff[p] + achunk(p, d) * cs
            send(in_ref.at[rows(other + at, cs)], rb0.at[rows(at, cs)], sem_of(0, p, d), partner)
    for d in order:
        for p in range(n_p):
            cs = 32 * units[p]
            at = hoff[p] + achunk(p, d) * cs
            copy(in_ref.at[rows(other + at, cs)], rb0.at[rows(at, cs)], sem_of(0, p, d), partner).wait_recv()
            h_ref[rows(at, cs), :] = in_ref[rows(mine + at, cs), :] + rb0[rows(at, cs), :]
            if d:
                send(h_ref.at[rows(at, cs)], rb1.at[pl.ds(off1[p] + (d - 1) * cs, cs)], sem_of(1, p, d), peer(AXES[p][0], d))
    for p in range(n_p):
        cs, us = 32 * units[p], 8 * units[p]
        own = hoff[p] + achunk(p, 0) * cs
        for d in (1, 3, 2):
            dst = rb1.at[pl.ds(off1[p] + (d - 1) * cs, cs)]
            copy(dst, dst, sem_of(1, p, d), partner).wait_recv()
        for d in order:
            b = bchunk(p, d) * us
            got = [rb1[rows(off1[p] + (e - 1) * cs + b, us), :] for e in (1, 2, 3)]
            p1[rows(offp1[p] + b, us), :] = (h_ref[rows(own + b, us), :] + got[1]) + (got[0] + got[2])
            if d:
                send(p1.at[rows(offp1[p] + b, us)], rb2.at[pl.ds(off2[p] + (d - 1) * us, us)], sem_of(2, p, d), peer(AXES[p][1], d))
    for p in range(n_p):
        us = 8 * units[p]
        for d in (1, 3, 2):
            dst = rb2.at[pl.ds(off2[p] + (d - 1) * us, us)]
            copy(dst, dst, sem_of(2, p, d), partner).wait_recv()
        got = [rb2[pl.ds(off2[p] + (e - 1) * us, us), :] for e in (1, 2, 3)]
        p2[pl.ds(offp2[p], us), :] = (p1[rows(offp1[p] + bchunk(p, 0) * us, us), :] + got[1]) + (got[0] + got[2])
        for d in (2, 1, 3):
            send(p2.at[pl.ds(offp2[p], us)], rb3.at[pl.ds(off2[p] + (d - 1) * us, us)], sem_of(3, p, d), peer(AXES[p][2], d))
    for p in range(n_p):
        us = 8 * units[p]
        for d in (1, 3, 2):
            dst = rb3.at[pl.ds(off2[p] + (d - 1) * us, us)]
            copy(dst, dst, sem_of(3, p, d), partner).wait_recv()
        got = [rb3[pl.ds(off2[p] + (e - 1) * us, us), :] for e in (1, 2, 3)]
        at = mine + hoff[p] + (achunk(p, 0) * 4 + bchunk(p, 0)) * us
        out_ref[rows(at, us), :] = (p2[pl.ds(offp2[p], us), :] + got[1]) + (got[0] + got[2])
        for d in (2, 1, 3):
            send(out_ref.at[rows(at, us)], out_ref.at[rows(at, us)], sem_of(4, p, d), peer(AXES[p][1], d))
    for p in range(n_p):
        cs, us = 32 * units[p], 8 * units[p]
        at = mine + hoff[p] + achunk(p, 0) * cs
        for d in (1, 3, 2):
            dst = out_ref.at[rows(at + bchunk(p, 4 - d) * us, us)]
            copy(dst, dst, sem_of(4, p, d), partner).wait_recv()
        for d in (2, 1, 3):
            send(out_ref.at[rows(at, cs)], out_ref.at[rows(at, cs)], sem_of(5, p, d), peer(AXES[p][0], d))
        send(out_ref.at[rows(at, cs)], out_ref.at[rows(at, cs)], sem_of(6, p, 0), partner)
    for d in (1, 3, 2):
        for p in range(n_p):
            cs = 32 * units[p]
            at = mine + hoff[p] + achunk(p, 4 - d) * cs
            dst = out_ref.at[rows(at, cs)]
            copy(dst, dst, sem_of(5, p, d), partner).wait_recv()
            send(dst, dst, sem_of(6, p, d), partner)
    for d in (0, 1, 3, 2):
        for p in range(n_p):
            cs = 32 * units[p]
            dst = out_ref.at[rows(other + hoff[p] + achunk(p, 4 - d if d else 0) * cs, cs)]
            copy(dst, dst, sem_of(6, p, d), partner).wait_recv()
    for c in sends:
        c.wait_send()


def all_sum(packed, units, cid):
    total = packed.shape[0]
    assert total == 2 * 16 * 8 * sum(units)
    su = 8 * sum(units)
    v = lambda r: pltpu.VMEM((r, 128), jnp.float32)
    n_sem = 7 * len(units) * 4
    return pl.pallas_call(
        functools.partial(ar_kernel, units),
        out_shape=jax.ShapeDtypeStruct((total, 128), jnp.float32),
        in_specs=[pl.BlockSpec(memory_space=pltpu.VMEM)],
        out_specs=pl.BlockSpec(memory_space=pltpu.VMEM),
        scratch_shapes=[v(16 * su), v(16 * su), v(12 * su), v(4 * su), v(3 * su), v(su), v(3 * su),
                        pltpu.SemaphoreType.DMA((n_sem,)), pltpu.SemaphoreType.DMA((n_sem,))],
        compiler_params=pltpu.CompilerParams(collective_id=cid, has_side_effects=True),
    )(packed)


def solution(mesh):
    def group_solve(a_blk, b_blk):
        b_wide = jnp.pad(b_blk, ((0, 0), (0, 64)))
        sum_one = all_sum(gram_first(a_blk), (6, 6, 6), 0)
        part_two, r_one, x_one = middle(sum_one, a_blk, b_wide)
        sum_two = all_sum(part_two, (7, 7, 6), 1)
        return last(sum_two, r_one, x_one)

    row_spec = P(("batch", "rows"), None)
    out_spec = P("batch", None)
    return jax.shard_map(group_solve, mesh=mesh, in_specs=(row_spec, row_spec), out_specs=(out_spec, out_spec), check_vma=False)
```
